32 devices in a mesh: wide: 8 (over z, y), narrow: 4 (over x, core).
Axes of the slice: x: 2, y: 2, z: 4, core: 2. Of those that a mesh axis runs over, the one named last changes fastest.
Arguments:
- inputs: bfloat16 [16384, 1024], P('wide', 'narrow'), may hold values from -6 to 6
- cotangent: bfloat16 [16384, 1024], P('wide', 'narrow'), may hold values from -6 to 6
- routing: int32 [16384], replicated, may hold values from 0 to 16383, as said below
- lengths: int32 [8, 4], P('wide'), may hold values from 1 to 1024, 2048 in all within a row
- ln1_gain: float32 [1024], P('narrow'), may hold values from 0.1 to 1.9
- ln1_bias: float32 [1024], P('narrow'), may hold values from -1.5 to 1.5
- qkv_weight: float32 [1024, 3, 1024], P('wide', None, 'narrow'), may hold values from -0.1875 to 0.1875
- qv_bias: float32 [2, 1024], P(None, 'narrow'), may hold values from -1.5 to 1.5
- out_weight: float32 [1024, 1024], P('narrow', 'wide'), may hold values from -1.5 to 1.5
- out_bias: float32 [1024], P('narrow'), may hold values from -1.5 to 1.5
- ln2_gain: float32 [1024], P('narrow'), may hold values from 0.1 to 1.9
- ln2_bias: float32 [1024], P('narrow'), may hold values from -1.5 to 1.5
- up_weight: float32 [1024, 4096], P('wide', 'narrow'), may hold values from -0.1875 to 0.1875
- up_bias: float32 [4096], P('narrow'), may hold values from -1.5 to 1.5
- down_weight: float32 [4096, 1024], P('narrow', 'wide'), may hold values from -0.09375 to 0.09375
- down_bias: float32 [1024], P('narrow'), may hold values from -1.5 to 1.5
Outputs:
- outputs: bfloat16 [16384, 1024], P('wide', 'narrow')
- input_grad: bfloat16 [16384, 1024], P('wide', 'narrow')
- ln1_gain_grad: float32 [1024], P('narrow')
- ln1_bias_grad: float32 [1024], P('narrow')
- qkv_weight_grad: float32 [1024, 3, 1024], P('wide', None, 'narrow')
- qv_bias_grad: float32 [2, 1024], P(None, 'narrow')
- out_weight_grad: float32 [1024, 1024], P('narrow', 'wide')
- out_bias_grad: float32 [1024], P('narrow')
- ln2_gain_grad: float32 [1024], P('narrow')
- ln2_bias_grad: float32 [1024], P('narrow')
- up_weight_grad: float32 [1024, 4096], P('wide', 'narrow')
- up_bias_grad: float32 [4096], P('narrow')
- down_weight_grad: float32 [4096, 1024], P('narrow', 'wide')
- down_bias_grad: float32 [1024], P('narrow')
The draws below stay inside these ranges and needn't reach their ends.
Inputs may be any that keep to these rules, and one draw needn't show every extreme that they name: routing is a permutation of the 16384 input rows; each aligned block of 2048 positions takes exactly 256 rows from each aligned block of 2048 input rows. Row w gives, in order, the lengths of the documents that fill positions w * 2048 to (w + 1) * 2048 - 1 of the routed order; each row sums to 2048.
All inputs are finite; a program needn't handle non-finite values.
Results may differ from the reference program's by a relative error of at most 0.012.
The reference program's roundings to bfloat16 on the way count: a program that leaves them out, or rounds other values in their place, can miss the bound.
Values may be sent and summed in bfloat16 or wider, within the bound.
A program may use at most 192 MiB of HBM per device.

```python
import math
import jax
import jax.numpy as jnp
import numpy as np
from jax import lax

D = 1024
HEADS = 16
HEAD_DIM = 64
FF = 4096
SEQ_MAX = 1024
TOK_DEV = 2048
DOCS = 4
TOKENS = 16384
N_WIDE = 8


def draw_routing(key, part):
    route_rows = TOK_DEV // N_WIDE
    source_key, target_key = jax.random.split(key)
    source_keys = jax.random.split(source_key, N_WIDE)
    shuffled_rows = jax.vmap(lambda one_key: jax.random.permutation(one_key, TOK_DEV))(source_keys)
    shuffled_rows = shuffled_rows.astype(jnp.int32).reshape(N_WIDE, N_WIDE, route_rows)
    offsets = jnp.arange(N_WIDE, dtype=jnp.int32)[:, None, None] * TOK_DEV
    slot_table = jnp.transpose(shuffled_rows + offsets, (1, 0, 2)).reshape(N_WIDE, TOK_DEV)
    target_keys = jax.random.split(target_key, N_WIDE)
    placed = jax.vmap(lambda one_key, slot_row: jax.random.permutation(one_key, slot_row))(target_keys, slot_table)
    return placed.reshape(N_WIDE * TOK_DEV).astype(jnp.int32)


def strengthened(array, own_key, source, target, shards_of, factor):
    owner, partner = [(jnp.arange(array.shape[dim]) // (array.shape[dim] // shards_of)).reshape([-1 if axis == dim else 1 for axis in range(array.ndim)]) for dim in (source, target)]
    chosen = jax.random.permutation(own_key, shards_of)[partner]
    strong = (owner == chosen) | (owner == (partner + shards_of // 2) % shards_of)
    return jnp.where(strong, factor * array, array)


def level_of(own_key, extent, shards, least, top_value):
    factor_of = 1.0
    for position, shards_of in shards:
        steps = jax.random.uniform(jax.random.fold_in(jax.random.fold_in(own_key, 6), position), (shards_of,), jnp.float32, least / len(shards), top_value / len(shards))
        factor_of = factor_of * jnp.repeat(jnp.exp(steps), extent[position] // shards_of).reshape((-1,) + (1,) * (len(extent) - 1 - position))
    return factor_of


def profile(number_of, total, bound, lean):
    weights = [(1 << 20) // math.isqrt(rank ** lean) + 1 for rank in range(2, number_of + 1)]
    spare, counts = total - bound - (number_of - 1), [1] * (number_of - 1)
    while spare > 0:
        movable = [i for i in range(number_of - 1) if counts[i] < bound]
        whole, budget = sum([weights[i] for i in movable]), spare
        for i in movable:
            more = min(bound - counts[i], max(1, budget * weights[i] // whole), spare)
            counts[i] = counts[i] + more
            spare = spare - more
    return np.array([bound] + counts)


def uneven_parts(own_key, count, total, most, skew):
    if count == 2:
        one = jax.random.randint(own_key, (), max(1, total - most), min(most, total - 1) + 1)
        return jnp.stack([one, total - one])
    sizes = jnp.asarray(profile(count, total, most, skew), jnp.int32)
    couples = (count - 1) // 2
    source_of, receiver = sizes[1:1 + 2 * couples:2], sizes[2:2 + 2 * couples:2]
    margin = jnp.minimum(source_of - 1, most - receiver)
    passed = jax.random.randint(jax.random.fold_in(own_key, 1), (couples,), 0, 1 << 20) % (margin + 1)
    sizes = sizes.at[1:1 + 2 * couples:2].set(source_of - passed).at[2:2 + 2 * couples:2].set(receiver + passed)
    return sizes[jax.random.permutation(jax.random.fold_in(own_key, 2), count)]


def noise(stream_key, shape, scale, most, cuts=(), kind=jnp.bfloat16):
    drawn = jax.random.normal(stream_key, shape, jnp.float32) * scale
    if len(cuts) > 0:
        drawn = level_of(stream_key, shape, cuts, -0.22, 0.18) * drawn
    return jnp.clip(drawn, min=-most, max=most).astype(kind)


def noise_with(rng, extent, width, reach, cuts, heavy, kind=jnp.bfloat16):
    values = width * jax.random.normal(rng, extent, jnp.float32)
    if cuts:
        values = values * level_of(rng, extent, cuts, -0.22, 0.18)
    return jnp.clip(strengthened(values, jax.random.fold_in(rng, 3), *heavy), -reach, reach).astype(kind)


def setup_inputs(seed: int = 0) -> dict:
    seeds = jax.random.split(jax.random.key(seed), 17)
    inputs = noise(seeds[0], (TOKENS, D), 1.0, 6.0, ((0, 8), (1, 4)))
    cotangent = noise_with(seeds[1], (TOKENS, D), 1.0, 6.0, ((0, 8), (1, 4)), (0, 1, 8, 2.0))
    routing = draw_routing(jax.random.fold_in(seeds[16], 71), 0)
    lengths = jax.vmap(lambda own: uneven_parts(own, DOCS, TOK_DEV, SEQ_MAX, 2))(jax.random.split(seeds[3], N_WIDE)).reshape((N_WIDE, DOCS)).astype(jnp.int32)
    ln1_gain = jnp.clip(1.0 + 0.18 * jax.random.normal(seeds[4], (D,), jnp.float32), 0.1, 1.9)
    ln1_bias = noise(seeds[5], (D,), 0.3, 1.5, ((0, 4),), jnp.float32)
    qkv_weight = noise(seeds[6], (D, 3, D), D ** -0.5, 0.1875, ((0, 8), (2, 4)), jnp.float32)
    qv_bias = noise(seeds[7], (2, D), 0.3, 1.5, ((1, 4),), jnp.float32)
    out_weight = noise(seeds[8], (D, D), (D // 64) ** -0.5, 1.5, ((0, 4), (1, 8)), jnp.float32)
    out_bias = noise(seeds[9], (D,), 0.3, 1.5, ((0, 4),), jnp.float32)
    ln2_gain = jnp.clip(1.0 + 0.18 * jax.random.normal(seeds[10], (D,), jnp.float32), 0.1, 1.9)
    ln2_bias = noise(seeds[11], (D,), 0.3, 1.5, ((0, 4),), jnp.float32)
    up_weight = noise(seeds[12], (D, FF), D ** -0.5, 0.1875, ((0, 8), (1, 4)), jnp.float32)
    up_bias = noise(seeds[13], (FF,), 0.3, 1.5, ((0, 4),), jnp.float32)
    down_weight = noise(seeds[14], (FF, D), FF ** -0.5, 0.09375, ((0, 4), (1, 8)), jnp.float32)
    down_bias = noise(seeds[15], (D,), 0.3, 1.5, ((0, 4),), jnp.float32)
    return {"inputs": inputs, "cotangent": cotangent, "routing": routing, "lengths": lengths, "ln1_gain": ln1_gain, "ln1_bias": ln1_bias, "qkv_weight": qkv_weight, "qv_bias": qv_bias, "out_weight": out_weight, "out_bias": out_bias, "ln2_gain": ln2_gain, "ln2_bias": ln2_bias, "up_weight": up_weight, "up_bias": up_bias, "down_weight": down_weight, "down_bias": down_bias}


@jax.custom_vjp
def low(v):
    return lax.optimization_barrier(v.astype(jnp.bfloat16)).astype(jnp.float32)

@jax.custom_vjp
def low_back(v):
    return v

def low_keep(v):
    return (low(v), None)

def low_pass(kept, grad):
    return (grad,)

def back_keep(v):
    return (v, None)

def back_low(kept, grad):
    return (low(grad),)
low.defvjp(low_keep, low_pass)
low_back.defvjp(back_keep, back_low)
NORM_EPS = 1e-05
HIGHEST_PREC = lax.Precision.HIGHEST

def round_both(values):
    return low(low_back(values))

def layer_norm(source, gain_vec, shift_vec):
    row_mean = lax.optimization_barrier(jnp.mean(source, axis=1, keepdims=True))
    row_var = lax.optimization_barrier(jnp.mean(source * source, axis=1, keepdims=True)) - row_mean * row_mean
    return (source - row_mean) * lax.rsqrt(row_var + NORM_EPS) * gain_vec + shift_vec

def segment_ids(doc_lengths, row_count):
    doc_ends = jnp.cumsum(doc_lengths)
    positions = jnp.arange(row_count, dtype=jnp.int32)
    return lax.optimization_barrier(jnp.sum((positions[:, None] >= doc_ends[None, :]).astype(jnp.int32), axis=1))

def attend(queries, key_rows, values, segment):
    row_count = queries.shape[0]
    block_rows = min(512, row_count)
    key_span = min(row_count, SEQ_MAX + block_rows)
    head_scale = HEAD_DIM ** (-0.5)

    def one_block(block_index):
        block_start = (block_index * block_rows).astype(jnp.int32)
        key_start = jnp.clip(block_start + block_rows - key_span, 0, row_count - key_span).astype(jnp.int32)
        query_block = lax.dynamic_slice_in_dim(queries, block_start, block_rows, 0)
        key_block = lax.dynamic_slice_in_dim(key_rows, key_start, key_span, 0)
        value_block = lax.dynamic_slice_in_dim(values, key_start, key_span, 0)
        query_pos = block_start + jnp.arange(block_rows, dtype=jnp.int32)
        key_pos = key_start + jnp.arange(key_span, dtype=jnp.int32)
        query_seg = lax.dynamic_slice_in_dim(segment, block_start, block_rows, 0)
        key_seg = lax.dynamic_slice_in_dim(segment, key_start, key_span, 0)
        allowed = (query_seg[:, None] == key_seg[None, :]) & (key_pos[None, :] <= query_pos[:, None])
        scores = low_back(jnp.einsum('qhd,khd->hqk', query_block, key_block, precision=HIGHEST_PREC) * head_scale)
        scores = jnp.where(allowed[None], scores, -1000000000.0)
        row_top = lax.optimization_barrier(jnp.max(scores, axis=2, keepdims=True))
        weights = jnp.exp(scores - row_top)
        attn_probs = weights / lax.optimization_barrier(jnp.sum(weights, axis=2, keepdims=True))
        return jnp.einsum('hqk,khd->qhd', low(attn_probs), value_block, precision=HIGHEST_PREC)
    blocks = lax.map(jax.checkpoint(one_block), jnp.arange(row_count // block_rows, dtype=jnp.int32))
    return blocks.reshape(queries.shape)

def device_forward(source, doc_lengths, params):
    gain_one, shift_one, qkv_mat, qv_shift, out_mat, out_shift, gain_two, shift_two, up_mat, up_shift, down_mat, down_shift = params
    row_count = source.shape[0]
    act_one = low(layer_norm(source, gain_one, shift_one))
    projected = jnp.einsum('td,dcf->tcf', act_one, qkv_mat, precision=HIGHEST_PREC)
    head_shape = (row_count, HEADS, HEAD_DIM)
    queries = round_both(projected[:, 0] + qv_shift[0]).reshape(head_shape)
    key_rows = round_both(projected[:, 1]).reshape(head_shape)
    values = round_both(projected[:, 2] + qv_shift[1]).reshape(head_shape)
    attended = attend(queries, key_rows, values, segment_ids(doc_lengths, row_count))
    attended = round_both(attended.reshape(row_count, D))
    branch = low_back(jnp.dot(attended, out_mat, precision=HIGHEST_PREC) + out_shift)
    middle = source + branch
    act_two = low(layer_norm(middle, gain_two, shift_two))
    preact = low_back(jnp.dot(act_two, up_mat, precision=HIGHEST_PREC) + up_shift)
    hidden = low(jax.nn.gelu(preact, approximate=True))
    return middle + jnp.dot(hidden, down_mat, precision=HIGHEST_PREC) + down_shift

def forward(source, routing, lengths, params):
    rounded = (params[0], params[1], low(params[2]), params[3], low(params[4]), params[5], params[6], params[7], low(params[8]), params[9], low(params[10]), params[11])
    routed = source[routing].reshape(N_WIDE, TOK_DEV, D)

    def device_step(carried, packed):
        return (carried, device_forward(packed[0], packed[1], rounded))
    _, results = lax.scan(jax.checkpoint(device_step), jnp.zeros((), jnp.float32), (routed, lengths))
    inverse = jnp.zeros((TOKENS,), jnp.int32).at[routing].set(jnp.arange(TOKENS, dtype=jnp.int32))
    return results.reshape(TOKENS, D)[inverse]

def reference(inputs, cotangent, routing, lengths, ln1_gain, ln1_bias, qkv_weight, qv_bias, out_weight, out_bias, ln2_gain, ln2_bias, up_weight, up_bias, down_weight, down_bias):
    params = (ln1_gain, ln1_bias, qkv_weight, qv_bias, out_weight, out_bias, ln2_gain, ln2_bias, up_weight, up_bias, down_weight, down_bias)

    def whole_layer(source, *weights):
        return forward(source, routing, lengths, weights)
    result, pullback = jax.vjp(whole_layer, inputs.astype(jnp.float32), *params)
    grads = pullback(cotangent.astype(jnp.float32))
    return (result.astype(jnp.bfloat16), grads[0].astype(jnp.bfloat16), grads[1], grads[2], grads[3], grads[4], grads[5], grads[6], grads[7], grads[8], grads[9], grads[10], grads[11], grads[12])
```

```python
import jax
import jax.numpy as jnp
from jax import lax
from jax.experimental import pallas as pl
from jax.experimental.pallas import tpu as pltpu
from jax.sharding import PartitionSpec as P

D = 1024
NORM_EPS = 1e-05

HEAD_DIM = 64
BLK = 256
NT = (((1,), (1,)), ((), ()))
NEG = -1e30


def head_mask(x, h):
    lane = lax.broadcasted_iota(jnp.int32, x.shape, 1)
    keep = (lane >= h * HEAD_DIM) & (lane < (h + 1) * HEAD_DIM)
    return jnp.where(keep, x, jnp.zeros_like(x))


def attn_fwd_kernel(first_ref, q_ref, k_ref, v_ref, start_ref, o_ref, lse_ref, s_ref, m_ref, l_ref, acc_ref):
    heads = q_ref.shape[1] // HEAD_DIM
    i = pl.program_id(0)
    lo = first_ref[i]
    q = q_ref[...] * jnp.bfloat16(HEAD_DIM ** -0.5)
    qs = [head_mask(q, h) for h in range(heads)]
    start = start_ref[...]
    q_pos = i * BLK + lax.broadcasted_iota(jnp.int32, (BLK, BLK), 0)
    k_iota = lax.broadcasted_iota(jnp.int32, (BLK, BLK), 1)
    m_ref[...] = jnp.full_like(m_ref, NEG)
    l_ref[...] = jnp.zeros_like(l_ref)
    acc_ref[...] = jnp.zeros_like(acc_ref)

    def scores(j, carry):
        rows = pl.ds(pl.multiple_of(j * BLK, BLK), BLK)
        kb = k_ref[rows, :]
        k_pos = j * BLK + k_iota
        allowed = (k_pos >= start[:, :1]) & (k_pos <= q_pos)
        for h in range(heads):
            s = lax.dot_general(qs[h], kb, NT, preferred_element_type=jnp.float32)
            s = jnp.where(allowed, s, NEG)
            s_ref[j - lo, h] = s
            m_ref[h] = jnp.maximum(m_ref[h], jnp.maximum(s[:, :128], s[:, 128:]))
        return carry

    lax.fori_loop(lo, i + 1, scores, 0)
    tops = []
    for h in range(heads):
        top = jnp.max(m_ref[h], axis=1, keepdims=True)
        tops.append(top)

    def mix(j, carry):
        rows = pl.ds(pl.multiple_of(j * BLK, BLK), BLK)
        vb = v_ref[rows, :]
        total = acc_ref[...]
        for h in range(heads):
            p = jnp.exp(s_ref[j - lo, h] - tops[h])
            l_ref[h] += p[:, :128] + p[:, 128:]
            total += jnp.dot(p.astype(jnp.bfloat16), head_mask(vb, h), preferred_element_type=jnp.float32)
        acc_ref[...] = total
        return carry

    lax.fori_loop(lo, i + 1, mix, 0)
    lane = lax.broadcasted_iota(jnp.int32, acc_ref.shape, 1)
    inv = jnp.zeros(acc_ref.shape, jnp.float32)
    column = lax.broadcasted_iota(jnp.int32, (BLK, 128), 1)
    sums = jnp.zeros((BLK, 128), jnp.float32)
    for h in range(heads):
        low = jnp.sum(l_ref[h], axis=1, keepdims=True)
        inv = jnp.where(lane // HEAD_DIM == h, 1.0 / low, inv)
        sums = jnp.where(column == h, tops[h] + jnp.log(low), sums)
    o_ref[...] = (acc_ref[...] * inv).astype(o_ref.dtype)
    lse_ref[...] = sums.T[:8]


def attention_forward(proj, first, start):
    rows = proj.shape[0]
    width = proj.shape[1] // 3
    heads = width // HEAD_DIM
    span = 1024 // BLK + 1
    return pl.pallas_call(
        attn_fwd_kernel,
        out_shape=(jax.ShapeDtypeStruct((rows, width), jnp.bfloat16), jax.ShapeDtypeStruct((8, rows), jnp.float32)),
        grid_spec=pltpu.PrefetchScalarGridSpec(
            num_scalar_prefetch=1,
            grid=(rows // BLK,),
            in_specs=[
                pl.BlockSpec((BLK, width), lambda i, f: (i, 0)),
                pl.BlockSpec((rows, width), lambda i, f: (0, 1)),
                pl.BlockSpec((rows, width), lambda i, f: (0, 2)),
                pl.BlockSpec((BLK, 128), lambda i, f: (i, 0)),
            ],
            out_specs=[
                pl.BlockSpec((BLK, width), lambda i, f: (i, 0)),
                pl.BlockSpec((8, BLK), lambda i, f: (0, i)),
            ],
            scratch_shapes=[
                pltpu.VMEM((span, heads, BLK, BLK), jnp.float32),
                pltpu.VMEM((heads, BLK, 128), jnp.float32),
                pltpu.VMEM((heads, BLK, 128), jnp.float32),
                pltpu.VMEM((BLK, width), jnp.float32),
            ],
        ),
        compiler_params=pltpu.CompilerParams(dimension_semantics=("arbitrary",), vmem_limit_bytes=40 << 20),
        cost_estimate=pl.CostEstimate(flops=16_000_000_000, bytes_accessed=8 << 20, transcendentals=0),
        name="attn_fwd",
    )(first, proj, proj, proj, start)


def attn_bwd_kernel(first_ref, q_ref, k_ref, v_ref, o_ref, do_ref, lse_ref, start_ref,
                    dq_ref, dk_ref, dv_ref, dk_acc, dv_acc, dq_acc, kt_ref):
    heads = q_ref.shape[1] // HEAD_DIM
    i = pl.program_id(0)
    lo = first_ref[i]

    @pl.when(i == 0)
    def _():
        dk_acc[...] = jnp.zeros_like(dk_acc)
        dv_acc[...] = jnp.zeros_like(dv_acc)
        kt_ref[...] = k_ref[...].T

    q = q_ref[...] * jnp.bfloat16(HEAD_DIM ** -0.5)
    do = do_ref[...]
    qs = [head_mask(q, h) for h in range(heads)]
    dos = [head_mask(do, h) for h in range(heads)]
    product = do.astype(jnp.float32) * o_ref[...].astype(jnp.float32)
    picker = (
        lax.broadcasted_iota(jnp.int32, (8, product.shape[1]), 1) // HEAD_DIM
        == lax.broadcasted_iota(jnp.int32, (8, product.shape[1]), 0)
    ).astype(jnp.float32)
    centre = lax.dot_general(picker, product, NT, preferred_element_type=jnp.float32, precision=lax.Precision.HIGHEST)
    lse = lse_ref[...]
    start = start_ref[...]
    k_iota = lax.broadcasted_iota(jnp.int32, (BLK, BLK), 0)
    q_pos = i * BLK + lax.broadcasted_iota(jnp.int32, (BLK, BLK), 1)
    dq_acc[...] = jnp.zeros_like(dq_acc)

    def pair(j, carry):
        at = pl.multiple_of(j * BLK, BLK)
        rows = pl.ds(at, BLK)
        kb = k_ref[rows, :]
        vb = v_ref[rows, :]
        k_pos = j * BLK + k_iota
        allowed = (k_pos >= start[:1, :]) & (k_pos <= q_pos)
        dk = dk_acc[rows, :]
        dv = dv_acc[rows, :]
        for h in range(heads):
            s = lax.dot_general(head_mask(kb, h), q, NT, preferred_element_type=jnp.float32)
            p = jnp.exp(jnp.where(allowed, s - lse[h:h + 1, :], NEG))
            dp = lax.dot_general(head_mask(vb, h), do, NT, preferred_element_type=jnp.float32)
            ds = (p * (dp - centre[h:h + 1, :])).astype(jnp.bfloat16)
            dv += jnp.dot(p.astype(jnp.bfloat16), dos[h], preferred_element_type=jnp.float32)
            dk += jnp.dot(ds, qs[h], preferred_element_type=jnp.float32)
            feats = slice(h * HEAD_DIM, (h + 1) * HEAD_DIM)
            dq_acc[feats, :] += jnp.dot(kt_ref[feats, rows], ds, preferred_element_type=jnp.float32)
        dk_acc[rows, :] = dk
        dv_acc[rows, :] = dv
        return carry

    lax.fori_loop(lo, i + 1, pair, 0)
    dq_ref[...] = (dq_acc[...].T * HEAD_DIM ** -0.5).astype(dq_ref.dtype)

    @pl.when(i == pl.num_programs(0) - 1)
    def _():
        dk_ref[...] = dk_acc[...].astype(dk_ref.dtype)
        dv_ref[...] = dv_acc[...].astype(dv_ref.dtype)


def attention_backward(proj, mixed, grad_mixed, lse, first, start_row):
    rows = proj.shape[0]
    width = proj.shape[1] // 3
    shape = jax.ShapeDtypeStruct((rows, width), jnp.bfloat16)
    tile = pl.BlockSpec((BLK, width), lambda i, f: (i, 0))
    whole = pl.BlockSpec((rows, width), lambda i, f: (0, 0))
    return pl.pallas_call(
        attn_bwd_kernel,
        out_shape=(shape, shape, shape),
        grid_spec=pltpu.PrefetchScalarGridSpec(
            num_scalar_prefetch=1,
            grid=(rows // BLK,),
            in_specs=[
                tile,
                pl.BlockSpec((rows, width), lambda i, f: (0, 1)),
                pl.BlockSpec((rows, width), lambda i, f: (0, 2)),
                tile,
                tile,
                pl.BlockSpec((8, BLK), lambda i, f: (0, i)),
                pl.BlockSpec((8, BLK), lambda i, f: (0, i)),
            ],
            out_specs=[tile, whole, whole],
            scratch_shapes=[
                pltpu.VMEM((rows, width), jnp.float32),
                pltpu.VMEM((rows, width), jnp.float32),
                pltpu.VMEM((width, BLK), jnp.float32),
                pltpu.VMEM((width, rows), jnp.bfloat16),
            ],
        ),
        compiler_params=pltpu.CompilerParams(dimension_semantics=("arbitrary",), vmem_limit_bytes=40 << 20),
        cost_estimate=pl.CostEstimate(flops=40_000_000_000, bytes_accessed=8 << 20, transcendentals=0),
        name="attn_bwd",
    )(first, proj, proj, proj, mixed, grad_mixed, lse, start_row)


def doc_tables(lengths_row, rows):
    ends = jnp.cumsum(lengths_row)
    starts = ends - lengths_row
    positions = jnp.arange(rows, dtype=jnp.int32)
    inside = (positions[:, None] >= starts[None, :]) & (positions[:, None] < ends[None, :])
    start = jnp.sum(jnp.where(inside, starts[None, :], 0), axis=1).astype(jnp.int32)
    first = start[::BLK] // BLK
    return start, first


def pick_kernel(index_ref, *refs):
    count = len(refs) // 2
    rows = refs[0].shape[0]
    column = index_ref[...].astype(jnp.float32).T[:, :1].astype(jnp.int32)
    source = lax.broadcasted_iota(jnp.int32, (BLK, rows), 1)
    chosen = jnp.where(source == column, 1.0, 0.0).astype(jnp.bfloat16)
    for x_ref, y_ref in zip(refs[:count], refs[count:]):
        y_ref[...] = jnp.dot(chosen, x_ref[...], preferred_element_type=jnp.float32).astype(y_ref.dtype)


def place_kernel(index_ref, *refs):
    count = len(refs) // 2
    rows = refs[0].shape[0]
    target = pl.program_id(0) * BLK + lax.broadcasted_iota(jnp.int32, (BLK, rows), 0)
    chosen = jnp.where(target == index_ref[:1, :], 1.0, 0.0).astype(jnp.bfloat16)
    for x_ref, y_ref in zip(refs[:count], refs[count:]):
        y_ref[...] = jnp.dot(chosen, x_ref[...], preferred_element_type=jnp.float32).astype(y_ref.dtype)


def permuted(kernel, name, index_rows, *arrays):
    rows = arrays[0].shape[0]
    picks = kernel is pick_kernel
    index_spec = pl.BlockSpec((8, BLK), lambda i: (0, i)) if picks else pl.BlockSpec((8, rows), lambda i: (0, 0))
    return pl.pallas_call(
        kernel,
        out_shape=[jax.ShapeDtypeStruct(a.shape, a.dtype) for a in arrays],
        grid=(rows // BLK,),
        in_specs=[index_spec] + [pl.BlockSpec(a.shape, lambda i: (0, 0)) for a in arrays],
        out_specs=[pl.BlockSpec((BLK, a.shape[1]), lambda i: (i, 0)) for a in arrays],
        compiler_params=pltpu.CompilerParams(dimension_semantics=("arbitrary",), vmem_limit_bytes=24 << 20),
        cost_estimate=pl.CostEstimate(flops=2 * rows * rows * 256 * len(arrays), bytes_accessed=4 << 20, transcendentals=0),
        name=name,
    )(index_rows, *arrays)


def pick(index_rows, *arrays):
    return permuted(pick_kernel, "pick_rows", index_rows, *arrays)


def place(index_rows, *arrays):
    return permuted(place_kernel, "place_rows", index_rows, *arrays)


def route_tables(routing, rows):
    groups = routing.shape[0] // rows
    me = lax.axis_index("wide")
    ids = routing.reshape(groups, rows)
    positions = jnp.arange(rows, dtype=jnp.int32)
    beyond = jnp.int32(rows * rows)
    keys = jnp.where(ids // rows == me, positions[None, :] * rows + ids % rows, beyond)
    send = (jnp.sort(keys, axis=1)[:, : rows // groups] % rows).reshape(rows)
    own = lax.dynamic_index_in_dim(ids, me, 0, keepdims=False)
    arrive = jnp.sort(own // rows * rows + positions) % rows
    return jnp.broadcast_to(send[None], (8, rows)), jnp.broadcast_to(arrive[None], (8, rows))


def exchanged(rows_out):
    return lax.all_to_all(rows_out, "wide", split_axis=0, concat_axis=0, tiled=True)


def row_stats(rows_full):
    mean = jnp.mean(rows_full, axis=1, keepdims=True)
    scale = lax.rsqrt(jnp.mean(rows_full * rows_full, axis=1, keepdims=True) - mean * mean + NORM_EPS)
    return mean, scale


def local(
    inputs,
    cotangent,
    routing,
    lengths,
    ln1_gain,
    ln1_bias,
    qkv_weight,
    qv_bias,
    out_weight,
    out_bias,
    ln2_gain,
    ln2_bias,
    up_weight,
    up_bias,
    down_weight,
    down_bias,
):
    low, wide_type = jnp.bfloat16, jnp.float32
    row_count, quarter = inputs.shape
    parts = lax.axis_size("narrow")
    share = row_count // parts
    part = lax.axis_index("narrow")
    send_rows, arrive_rows = route_tables(routing, row_count)

    def mine(rows_full):
        return lax.dynamic_slice_in_dim(rows_full, part * share, share, 0)

    def my_features(rows_full):
        return lax.dynamic_slice_in_dim(rows_full, part * quarter, quarter, 1)

    (sent,) = pick(send_rows, inputs)
    (routed,) = place(arrive_rows, exchanged(sent))
    (sent_grad,) = pick(send_rows, cotangent)
    (routed_grad,) = place(arrive_rows, exchanged(sent_grad))
    vectors = jnp.stack([ln1_gain, ln1_bias, ln2_gain, ln2_bias, out_bias, down_bias])
    vectors = lax.all_gather(vectors, "narrow", axis=1, tiled=True)
    start, first = doc_tables(lengths[0], row_count)

    qkv_full = lax.all_gather(qkv_weight.astype(low).reshape(qkv_weight.shape[0], 3 * quarter), "wide", axis=0, tiled=True)
    out_full = lax.all_gather(out_weight.astype(low), "wide", axis=1, tiled=True)
    up_full = lax.all_gather(up_weight.astype(low), "wide", axis=0, tiled=True)
    down_full = lax.all_gather(down_weight.astype(low), "wide", axis=1, tiled=True)

    routed_full = lax.all_gather(routed, "narrow", axis=1, tiled=True).astype(wide_type)
    mean_one, scale_one = row_stats(routed_full)
    act_one = ((routed_full - mean_one) * scale_one * vectors[0] + vectors[1]).astype(low)
    shift = jnp.concatenate([qv_bias[0], jnp.zeros((quarter,), wide_type), qv_bias[1]])
    proj = (jnp.dot(act_one, qkv_full, preferred_element_type=wide_type) + shift).astype(low)
    mixed, log_sums = attention_forward(proj, first, jnp.broadcast_to(start[:, None], (row_count, 128)))
    branch = jnp.dot(mixed, out_full, preferred_element_type=wide_type).astype(low)
    branch = lax.psum_scatter(branch, "narrow", scatter_dimension=0, tiled=True).astype(wide_type)
    middle = mine(routed_full) + branch + vectors[4]
    mean_two, scale_two = row_stats(middle)
    normed_two = (middle - mean_two) * scale_two
    act_two = lax.all_gather((normed_two * vectors[2] + vectors[3]).astype(low), "narrow", axis=0, tiled=True)

    grad_full = lax.all_gather(routed_grad, "narrow", axis=1, tiled=True)
    preact = jnp.dot(act_two, up_full, preferred_element_type=wide_type) + up_bias
    gelu, gelu_back = jax.vjp(lambda u: jax.nn.gelu(u, approximate=True), preact)
    hidden = gelu.astype(low)
    grad_hidden = jnp.einsum("td,fd->tf", grad_full, down_full, preferred_element_type=wide_type)
    grad_pre = gelu_back(grad_hidden)[0].astype(low)
    grad_act_two = jnp.einsum("tf,df->td", grad_pre, up_full, preferred_element_type=wide_type).astype(low)
    grad_act_two = lax.psum_scatter(grad_act_two, "narrow", scatter_dimension=0, tiled=True).astype(wide_type)
    scaled = grad_act_two * vectors[2]
    back_two = scale_two * (
        scaled
        - jnp.mean(scaled, axis=1, keepdims=True)
        - normed_two * jnp.mean(scaled * normed_two, axis=1, keepdims=True)
    )
    grad_branch = (mine(grad_full).astype(wide_type) + back_two).astype(low)
    branch_full = lax.all_gather(grad_branch, "narrow", axis=0, tiled=True)
    gain_two_grad = jnp.sum(grad_act_two * normed_two, axis=0)
    bias_two_grad = jnp.sum(grad_act_two, axis=0)

    held = jnp.arange(parts, dtype=jnp.int32)[:, None, None] == part
    kept = jnp.where(held, (middle + vectors[5])[None], 0.0).reshape(row_count, D)
    result = (jnp.dot(hidden, down_full, preferred_element_type=wide_type) + kept).astype(low)
    result = lax.psum_scatter(result, "narrow", scatter_dimension=1, tiled=True)
    down_grad = jnp.einsum("tf,td->fd", hidden, grad_full, preferred_element_type=wide_type).astype(low)
    up_grad = jnp.einsum("td,tf->df", act_two, grad_pre, preferred_element_type=wide_type).astype(low)
    down_grad = lax.psum_scatter(down_grad, "wide", scatter_dimension=1, tiled=True).astype(wide_type)
    up_grad = lax.psum_scatter(up_grad, "wide", scatter_dimension=0, tiled=True).astype(wide_type)

    out_grad = jnp.einsum("tf,td->fd", mixed, branch_full, preferred_element_type=wide_type).astype(low)
    out_grad = lax.psum_scatter(out_grad, "wide", scatter_dimension=1, tiled=True).astype(wide_type)
    grad_mixed = jnp.einsum("td,fd->tf", branch_full, out_full, preferred_element_type=wide_type).astype(low)
    grad_q, grad_k, grad_v = attention_backward(
        proj, mixed, grad_mixed, log_sums, first, jnp.broadcast_to(start[None], (8, row_count))
    )
    grad_proj = jnp.concatenate([grad_q, grad_k, grad_v], axis=1)
    grad_act_one = jnp.einsum("tc,dc->td", grad_proj, qkv_full, preferred_element_type=wide_type).astype(low)
    grad_act_one = lax.psum_scatter(grad_act_one, "narrow", scatter_dimension=1, tiled=True).astype(wide_type)
    qkv_grad = jnp.einsum("td,tc->dc", act_one, grad_proj, preferred_element_type=wide_type).astype(low)
    qkv_grad = lax.psum_scatter(qkv_grad, "wide", scatter_dimension=0, tiled=True).astype(wide_type)

    normed_one = (routed.astype(wide_type) - mean_one) * scale_one
    scaled = grad_act_one * ln1_gain
    totals = lax.psum(jnp.stack([jnp.sum(scaled, axis=1), jnp.sum(scaled * normed_one, axis=1)]), "narrow") / D
    back_one = scale_one * (scaled - totals[0][:, None] - normed_one * totals[1][:, None])
    grad_input = (my_features(branch_full).astype(wide_type) + back_one).astype(low)

    (result_sent,) = pick(arrive_rows, result)
    (outputs,) = place(send_rows, exchanged(result_sent))
    (input_sent,) = pick(arrive_rows, grad_input)
    (input_grad,) = place(send_rows, exchanged(input_sent))

    norm_two = lax.psum(jnp.stack([gain_two_grad, bias_two_grad]), ("wide", "narrow"))
    norm_two = lax.dynamic_slice_in_dim(norm_two, part * quarter, quarter, 1)
    middle_sums = lax.psum(
        (
            jnp.sum(my_features(branch_full), axis=0, dtype=wide_type),
            jnp.sum(grad_pre, axis=0, dtype=wide_type),
            jnp.sum(routed_grad, axis=0, dtype=wide_type),
        ),
        "wide",
    )
    last_sums = lax.psum(
        (
            jnp.sum(grad_act_one * normed_one, axis=0),
            jnp.sum(grad_act_one, axis=0),
            jnp.stack([jnp.sum(grad_q, axis=0, dtype=wide_type), jnp.sum(grad_v, axis=0, dtype=wide_type)]),
        ),
        "wide",
    )
    return (
        outputs,
        input_grad,
        last_sums[0],
        last_sums[1],
        qkv_grad.reshape(qkv_weight.shape),
        last_sums[2],
        out_grad,
        middle_sums[0],
        norm_two[0],
        norm_two[1],
        up_grad,
        middle_sums[1],
        down_grad,
        middle_sums[2],
    )


def solution(mesh):
    row_mat, col_mat, vector = P("wide", "narrow"), P("narrow", "wide"), P("narrow")
    projections, pair = P("wide", None, "narrow"), P(None, "narrow")
    return jax.shard_map(
        local,
        mesh=mesh,
        in_specs=(
            row_mat,
            row_mat,
            P(),
            P("wide", None),
            vector,
            vector,
            projections,
            pair,
            col_mat,
            vector,
            vector,
            vector,
            row_mat,
            vector,
            col_mat,
            vector,
        ),
        out_specs=(
            row_mat,
            row_mat,
            vector,
            vector,
            projections,
            pair,
            col_mat,
            vector,
            vector,
            vector,
            row_mat,
            vector,
            col_mat,
            vector,
        ),
        check_vma=False,
    )
```

```python
import functools

import jax
import jax.numpy as jnp
from jax import lax
from jax.experimental import pallas as pl
from jax.experimental.pallas import tpu as pltpu
from jax.sharding import PartitionSpec as P

D = 1024
NORM_EPS = 1e-05

HEAD_DIM = 64
BLK = 256
NT = (((1,), (1,)), ((), ()))
NEG = -1e30


def head_mask(x, h):
    lane = lax.broadcasted_iota(jnp.int32, x.shape, 1)
    keep = (lane >= h * HEAD_DIM) & (lane < (h + 1) * HEAD_DIM)
    return jnp.where(keep, x, jnp.zeros_like(x))


def attn_fwd_kernel(first_ref, q_ref, k_ref, v_ref, start_ref, o_ref, lse_ref, s_ref, m_ref, l_ref, acc_ref):
    heads = q_ref.shape[1] // HEAD_DIM
    i = pl.program_id(0)
    lo = first_ref[i]
    q = q_ref[...] * jnp.bfloat16(HEAD_DIM ** -0.5)
    qs = [head_mask(q, h) for h in range(heads)]
    start = start_ref[...]
    q_pos = i * BLK + lax.broadcasted_iota(jnp.int32, (BLK, BLK), 0)
    k_iota = lax.broadcasted_iota(jnp.int32, (BLK, BLK), 1)
    m_ref[...] = jnp.full_like(m_ref, NEG)
    l_ref[...] = jnp.zeros_like(l_ref)
    acc_ref[...] = jnp.zeros_like(acc_ref)

    def scores(j, carry):
        rows = pl.ds(pl.multiple_of(j * BLK, BLK), BLK)
        kb = k_ref[rows, :]
        k_pos = j * BLK + k_iota
        allowed = (k_pos >= start[:, :1]) & (k_pos <= q_pos)
        for h in range(heads):
            s = lax.dot_general(qs[h], kb, NT, preferred_element_type=jnp.float32)
            s = jnp.where(allowed, s, NEG)
            s_ref[j - lo, h] = s
            m_ref[h] = jnp.maximum(m_ref[h], jnp.maximum(s[:, :128], s[:, 128:]))
        return carry

    lax.fori_loop(lo, i + 1, scores, 0)
    tops = []
    for h in range(heads):
        top = jnp.max(m_ref[h], axis=1, keepdims=True)
        tops.append(top)

    def mix(j, carry):
        rows = pl.ds(pl.multiple_of(j * BLK, BLK), BLK)
        vb = v_ref[rows, :]
        total = acc_ref[...]
        for h in range(heads):
            p = jnp.exp(s_ref[j - lo, h] - tops[h])
            l_ref[h] += p[:, :128] + p[:, 128:]
            total += jnp.dot(p.astype(jnp.bfloat16), head_mask(vb, h), preferred_element_type=jnp.float32)
        acc_ref[...] = total
        return carry

    lax.fori_loop(lo, i + 1, mix, 0)
    lane = lax.broadcasted_iota(jnp.int32, acc_ref.shape, 1)
    inv = jnp.zeros(acc_ref.shape, jnp.float32)
    column = lax.broadcasted_iota(jnp.int32, (BLK, 128), 1)
    sums = jnp.zeros((BLK, 128), jnp.float32)
    for h in range(heads):
        low = jnp.sum(l_ref[h], axis=1, keepdims=True)
        inv = jnp.where(lane // HEAD_DIM == h, 1.0 / low, inv)
        sums = jnp.where(column == h, tops[h] + jnp.log(low), sums)
    o_ref[...] = (acc_ref[...] * inv).astype(o_ref.dtype)
    lse_ref[...] = sums.T[:8]


def attention_forward(proj, first, start):
    rows = proj.shape[0]
    width = proj.shape[1] // 3
    heads = width // HEAD_DIM
    span = 1024 // BLK + 1
    return pl.pallas_call(
        attn_fwd_kernel,
        out_shape=(jax.ShapeDtypeStruct((rows, width), jnp.bfloat16), jax.ShapeDtypeStruct((8, rows), jnp.float32)),
        grid_spec=pltpu.PrefetchScalarGridSpec(
            num_scalar_prefetch=1,
            grid=(rows // BLK,),
            in_specs=[
                pl.BlockSpec((BLK, width), lambda i, f: (i, 0)),
                pl.BlockSpec((rows, width), lambda i, f: (0, 1)),
                pl.BlockSpec((rows, width), lambda i, f: (0, 2)),
                pl.BlockSpec((BLK, 128), lambda i, f: (i, 0)),
            ],
            out_specs=[
                pl.BlockSpec((BLK, width), lambda i, f: (i, 0)),
                pl.BlockSpec((8, BLK), lambda i, f: (0, i)),
            ],
            scratch_shapes=[
                pltpu.VMEM((span, heads, BLK, BLK), jnp.float32),
                pltpu.VMEM((heads, BLK, 128), jnp.float32),
                pltpu.VMEM((heads, BLK, 128), jnp.float32),
                pltpu.VMEM((BLK, width), jnp.float32),
            ],
        ),
        compiler_params=pltpu.CompilerParams(dimension_semantics=("arbitrary",), vmem_limit_bytes=40 << 20),
        cost_estimate=pl.CostEstimate(flops=16_000_000_000, bytes_accessed=8 << 20, transcendentals=0),
        name="attn_fwd",
    )(first, proj, proj, proj, start)


def attn_bwd_kernel(first_ref, q_ref, k_ref, v_ref, o_ref, do_ref, lse_ref, start_ref,
                    dq_ref, dk_ref, dv_ref, dk_acc, dv_acc, dq_acc, kt_ref):
    heads = q_ref.shape[1] // HEAD_DIM
    i = pl.program_id(0)
    lo = first_ref[i]

    @pl.when(i == 0)
    def _():
        dk_acc[...] = jnp.zeros_like(dk_acc)
        dv_acc[...] = jnp.zeros_like(dv_acc)
        kt_ref[...] = k_ref[...].T

    q = q_ref[...] * jnp.bfloat16(HEAD_DIM ** -0.5)
    do = do_ref[...]
    qs = [head_mask(q, h) for h in range(heads)]
    dos = [head_mask(do, h) for h in range(heads)]
    product = do.astype(jnp.float32) * o_ref[...].astype(jnp.float32)
    picker = (
        lax.broadcasted_iota(jnp.int32, (8, product.shape[1]), 1) // HEAD_DIM
        == lax.broadcasted_iota(jnp.int32, (8, product.shape[1]), 0)
    ).astype(jnp.float32)
    centre = lax.dot_general(picker, product, NT, preferred_element_type=jnp.float32, precision=lax.Precision.HIGHEST)
    lse = lse_ref[...]
    start = start_ref[...]
    k_iota = lax.broadcasted_iota(jnp.int32, (BLK, BLK), 0)
    q_pos = i * BLK + lax.broadcasted_iota(jnp.int32, (BLK, BLK), 1)
    dq_acc[...] = jnp.zeros_like(dq_acc)

    def pair(j, carry):
        at = pl.multiple_of(j * BLK, BLK)
        rows = pl.ds(at, BLK)
        kb = k_ref[rows, :]
        vb = v_ref[rows, :]
        k_pos = j * BLK + k_iota
        allowed = (k_pos >= start[:1, :]) & (k_pos <= q_pos)
        dk = dk_acc[rows, :]
        dv = dv_acc[rows, :]
        for h in range(heads):
            s = lax.dot_general(head_mask(kb, h), q, NT, preferred_element_type=jnp.float32)
            p = jnp.exp(jnp.where(allowed, s - lse[h:h + 1, :], NEG))
            dp = lax.dot_general(head_mask(vb, h), do, NT, preferred_element_type=jnp.float32)
            ds = (p * (dp - centre[h:h + 1, :])).astype(jnp.bfloat16)
            dv += jnp.dot(p.astype(jnp.bfloat16), dos[h], preferred_element_type=jnp.float32)
            dk += jnp.dot(ds, qs[h], preferred_element_type=jnp.float32)
            feats = slice(h * HEAD_DIM, (h + 1) * HEAD_DIM)
            dq_acc[feats, :] += jnp.dot(kt_ref[feats, rows], ds, preferred_element_type=jnp.float32)
        dk_acc[rows, :] = dk
        dv_acc[rows, :] = dv
        return carry

    lax.fori_loop(lo, i + 1, pair, 0)
    dq_ref[...] = (dq_acc[...].T * HEAD_DIM ** -0.5).astype(dq_ref.dtype)

    @pl.when(i == pl.num_programs(0) - 1)
    def _():
        dk_ref[...] = dk_acc[...].astype(dk_ref.dtype)
        dv_ref[...] = dv_acc[...].astype(dv_ref.dtype)


def attention_backward(proj, mixed, grad_mixed, lse, first, start_row):
    rows = proj.shape[0]
    width = proj.shape[1] // 3
    shape = jax.ShapeDtypeStruct((rows, width), jnp.bfloat16)
    tile = pl.BlockSpec((BLK, width), lambda i, f: (i, 0))
    whole = pl.BlockSpec((rows, width), lambda i, f: (0, 0))
    return pl.pallas_call(
        attn_bwd_kernel,
        out_shape=(shape, shape, shape),
        grid_spec=pltpu.PrefetchScalarGridSpec(
            num_scalar_prefetch=1,
            grid=(rows // BLK,),
            in_specs=[
                tile,
                pl.BlockSpec((rows, width), lambda i, f: (0, 1)),
                pl.BlockSpec((rows, width), lambda i, f: (0, 2)),
                tile,
                tile,
                pl.BlockSpec((8, BLK), lambda i, f: (0, i)),
                pl.BlockSpec((8, BLK), lambda i, f: (0, i)),
            ],
            out_specs=[tile, whole, whole],
            scratch_shapes=[
                pltpu.VMEM((rows, width), jnp.float32),
                pltpu.VMEM((rows, width), jnp.float32),
                pltpu.VMEM((width, BLK), jnp.float32),
                pltpu.VMEM((width, rows), jnp.bfloat16),
            ],
        ),
        compiler_params=pltpu.CompilerParams(dimension_semantics=("arbitrary",), vmem_limit_bytes=40 << 20),
        cost_estimate=pl.CostEstimate(flops=40_000_000_000, bytes_accessed=8 << 20, transcendentals=0),
        name="attn_bwd",
    )(first, proj, proj, proj, mixed, grad_mixed, lse, start_row)


def doc_tables(lengths_row, rows):
    ends = jnp.cumsum(lengths_row)
    starts = ends - lengths_row
    positions = jnp.arange(rows, dtype=jnp.int32)
    inside = (positions[:, None] >= starts[None, :]) & (positions[:, None] < ends[None, :])
    start = jnp.sum(jnp.where(inside, starts[None, :], 0), axis=1).astype(jnp.int32)
    first = start[::BLK] // BLK
    return start, first


MESH = pl.DeviceIdType.MESH


def neighbours():
    own = lax.axis_index("narrow")
    beside = own + 1 - 2 * (own % 2)
    across = (own + 2) % 4
    return own, beside, across, (beside + 2) % 4


def greet(*peers):
    barrier = pltpu.get_barrier_semaphore()
    for peer in peers:
        pl.semaphore_signal(barrier, inc=1, device_id={"narrow": peer}, device_id_type=MESH)
    pl.semaphore_wait(barrier, len(peers))


def push(src, dst, send_sem, recv_sem, peer):
    return pltpu.make_async_remote_copy(
        src_ref=src, dst_ref=dst, send_sem=send_sem, recv_sem=recv_sem, device_id={"narrow": peer}, device_id_type=MESH
    )


def chunk(base, k, rows):
    return pl.ds(pl.multiple_of(base + k * rows, rows), rows)


def rows_norm(x):
    mean = jnp.mean(x, axis=1, keepdims=True)
    scale = lax.rsqrt(jnp.mean(x * x, axis=1, keepdims=True) - mean * mean + NORM_EPS)
    return (x - mean) * scale, scale


def project_kernel(rows, mixed_ref, weight_ref, routed_ref, vec_ref, act_ref, middle_ref,
                   a_out, a_in, x_out, x_in, b_out, b_in, sends, recvs):
    own, beside, across, corner = neighbours()
    share = middle_ref.shape[0]
    count = share // rows
    greet(beside, across)

    def partial(quarter, k):
        at = chunk(quarter * share, k, rows)
        return jnp.dot(mixed_ref[at, :], weight_ref[...], preferred_element_type=jnp.float32)

    def copies(kind, k, src, dst, peer):
        at = chunk(0, k, rows)
        return push(src.at[at, :], dst.at[at, :], sends.at[kind, k], recvs.at[kind, k], peer)

    def spread(kind, quarter, k, peer):
        at = chunk(quarter * share, k, rows)
        return push(act_ref.at[at, :], act_ref.at[at, :], sends.at[kind, k], recvs.at[kind, k], peer)

    def first(k, carry):
        a_out[chunk(0, k, rows), :] = partial(corner, k).astype(jnp.bfloat16)
        copies(0, k, a_out, a_in, beside).start()
        return carry

    def second(k, carry):
        part = partial(across, k)
        copies(0, k, a_out, a_in, beside).wait_recv()
        at = chunk(0, k, rows)
        x_out[at, :] = (part + a_in[at, :].astype(jnp.float32)).astype(jnp.bfloat16)
        copies(1, k, x_out, x_in, across).start()
        return carry

    def third(k, carry):
        b_out[chunk(0, k, rows), :] = partial(beside, k).astype(jnp.bfloat16)
        copies(2, k, b_out, b_in, beside).start()
        return carry

    def fourth(k, carry):
        part = partial(own, k)
        at = chunk(0, k, rows)
        copies(2, k, b_out, b_in, beside).wait_recv()
        part += b_in[at, :].astype(jnp.float32)
        copies(1, k, x_out, x_in, across).wait_recv()
        part += x_in[at, :].astype(jnp.float32)
        middle = part + routed_ref[at, :].astype(jnp.float32) + vec_ref[0:1, :]
        middle_ref[at, :] = middle
        normed, _ = rows_norm(middle)
        act_ref[chunk(own * share, k, rows), :] = (normed * vec_ref[1:2, :] + vec_ref[2:3, :]).astype(jnp.bfloat16)
        spread(3, own, k, across).start()
        spread(4, own, k, beside).start()
        return carry

    def fifth(k, carry):
        spread(3, across, k, across).wait_recv()
        spread(5, across, k, beside).start()
        return carry

    def last(k, carry):
        copies(0, k, a_out, a_in, beside).wait_send()
        copies(1, k, x_out, x_in, across).wait_send()
        copies(2, k, b_out, b_in, beside).wait_send()
        spread(3, own, k, across).wait_send()
        spread(4, own, k, beside).wait_send()
        spread(5, across, k, beside).wait_send()
        spread(4, beside, k, beside).wait_recv()
        spread(5, corner, k, beside).wait_recv()
        return carry

    for stage in (first, second, third, fourth, fifth, last):
        lax.fori_loop(0, count, stage, 0)


def project_and_norm(mixed, out_full, routed_mine, vectors, rows=128):
    total, width = mixed.shape[0], out_full.shape[1]
    share = routed_mine.shape[0]
    count = share // rows
    buffer = pltpu.VMEM((share, width), jnp.bfloat16)
    vmem = pl.BlockSpec(memory_space=pltpu.VMEM)
    return pl.pallas_call(
        functools.partial(project_kernel, rows),
        out_shape=(
            jax.ShapeDtypeStruct((total, width), jnp.bfloat16),
            jax.ShapeDtypeStruct((share, width), jnp.float32),
        ),
        in_specs=[vmem] * 4,
        out_specs=(vmem, vmem),
        scratch_shapes=[buffer] * 6 + [pltpu.SemaphoreType.DMA((6, count)), pltpu.SemaphoreType.DMA((6, count))],
        compiler_params=pltpu.CompilerParams(collective_id=1, has_side_effects=True, vmem_limit_bytes=40 << 20),
        cost_estimate=pl.CostEstimate(flops=30_000_000_000, bytes_accessed=16 << 20, transcendentals=0),
        name="project_and_norm",
    )(mixed, out_full, routed_mine, vectors)


GELU_A = (2.0 / 3.141592653589793) ** 0.5
GELU_B = 0.044715


def mlp_kernel(rows, act_ref, grad_ref, up_ref, down_ref, bias_ref, middle_ref, vec_ref,
               hidden_ref, gpre_ref, branch_ref, norm_ref,
               a_out, a_in, x_out, x_in, b_out, b_in, sends, recvs):
    own, beside, across, corner = neighbours()
    share = middle_ref.shape[0]
    count = share // rows
    greet(beside, across)
    norm_ref[...] = jnp.zeros_like(norm_ref)

    def partial(quarter, k):
        at = chunk(quarter * share, k, rows)
        u = jnp.dot(act_ref[at, :], up_ref[...], preferred_element_type=jnp.float32) + bias_ref[0:1, :]
        square = u * u
        t = jnp.tanh(GELU_A * (u + GELU_B * square * u))
        half = 0.5 * (1.0 + t)
        hidden_ref[at, :] = (u * half).astype(jnp.bfloat16)
        slope = half + 0.5 * u * (1.0 - t * t) * (GELU_A * (1.0 + (3.0 * GELU_B) * square))
        back = lax.dot_general(grad_ref[at, :], down_ref[...], NT, preferred_element_type=jnp.float32)
        gpre = (back * slope).astype(jnp.bfloat16)
        gpre_ref[at, :] = gpre
        return lax.dot_general(gpre, up_ref[...], NT, preferred_element_type=jnp.float32)

    def copies(kind, k, src, dst, peer):
        at = chunk(0, k, rows)
        return push(src.at[at, :], dst.at[at, :], sends.at[kind, k], recvs.at[kind, k], peer)

    def spread(kind, quarter, k, peer):
        at = chunk(quarter * share, k, rows)
        return push(branch_ref.at[at, :], branch_ref.at[at, :], sends.at[kind, k], recvs.at[kind, k], peer)

    def outward(k, carry):
        at = chunk(0, k, rows)
        a_out[at, :] = partial(corner, k).astype(jnp.bfloat16)
        copies(0, k, a_out, a_in, beside).start()
        part = partial(across, k)
        copies(0, k, a_out, a_in, beside).wait_recv()
        x_out[at, :] = (part + a_in[at, :].astype(jnp.float32)).astype(jnp.bfloat16)
        copies(1, k, x_out, x_in, across).start()
        return carry

    def inward(k, carry):
        at = chunk(0, k, rows)
        b_out[at, :] = partial(beside, k).astype(jnp.bfloat16)
        copies(2, k, b_out, b_in, beside).start()
        part = partial(own, k)
        copies(2, k, b_out, b_in, beside).wait_recv()
        part += b_in[at, :].astype(jnp.float32)
        copies(1, k, x_out, x_in, across).wait_recv()
        part += x_in[at, :].astype(jnp.float32)
        normed, scale = rows_norm(middle_ref[at, :])
        norm_ref[0:1, :] += jnp.sum(part * normed, axis=0, keepdims=True)
        norm_ref[1:2, :] += jnp.sum(part, axis=0, keepdims=True)
        scaled = part * vec_ref[1:2, :]
        back = scale * (
            scaled
            - jnp.mean(scaled, axis=1, keepdims=True)
            - normed * jnp.mean(scaled * normed, axis=1, keepdims=True)
        )
        rows_own = chunk(own * share, k, rows)
        branch_ref[rows_own, :] = (grad_ref[rows_own, :].astype(jnp.float32) + back).astype(jnp.bfloat16)
        spread(3, own, k, across).start()
        spread(4, own, k, beside).start()
        return carry

    def forward(k, carry):
        spread(3, across, k, across).wait_recv()
        spread(5, across, k, beside).start()
        return carry

    def last(k, carry):
        copies(0, k, a_out, a_in, beside).wait_send()
        copies(1, k, x_out, x_in, across).wait_send()
        copies(2, k, b_out, b_in, beside).wait_send()
        spread(3, own, k, across).wait_send()
        spread(4, own, k, beside).wait_send()
        spread(5, across, k, beside).wait_send()
        spread(4, beside, k, beside).wait_recv()
        spread(5, corner, k, beside).wait_recv()
        return carry

    for stage in (outward, inward, forward, last):
        lax.fori_loop(0, count, stage, 0)


def mlp_both_ways(act_two, grad_full, up_full, down_full, up_bias, middle, vectors, rows=256):
    total, width = act_two.shape
    hidden = up_full.shape[1]
    share = middle.shape[0]
    count = share // rows
    buffer = pltpu.VMEM((share, width), jnp.bfloat16)
    vmem = pl.BlockSpec(memory_space=pltpu.VMEM)
    return pl.pallas_call(
        functools.partial(mlp_kernel, rows),
        out_shape=(
            jax.ShapeDtypeStruct((total, hidden), jnp.bfloat16),
            jax.ShapeDtypeStruct((total, hidden), jnp.bfloat16),
            jax.ShapeDtypeStruct((total, width), jnp.bfloat16),
            jax.ShapeDtypeStruct((8, width), jnp.float32),
        ),
        in_specs=[vmem] * 7,
        out_specs=(vmem,) * 4,
        scratch_shapes=[buffer] * 6 + [pltpu.SemaphoreType.DMA((6, count)), pltpu.SemaphoreType.DMA((6, count))],
        compiler_params=pltpu.CompilerParams(collective_id=2, has_side_effects=True, vmem_limit_bytes=60 << 20),
        cost_estimate=pl.CostEstimate(flops=40_000_000_000, bytes_accessed=32 << 20, transcendentals=0),
        name="mlp_both_ways",
    )(act_two, grad_full, up_full, down_full, up_bias, middle, vectors)


def pick_kernel(index_ref, *refs):
    count = len(refs) // 2
    rows = refs[0].shape[0]
    column = index_ref[...].astype(jnp.float32).T[:, :1].astype(jnp.int32)
    source = lax.broadcasted_iota(jnp.int32, (BLK, rows), 1)
    chosen = jnp.where(source == column, 1.0, 0.0).astype(jnp.bfloat16)
    for x_ref, y_ref in zip(refs[:count], refs[count:]):
        y_ref[...] = jnp.dot(chosen, x_ref[...], preferred_element_type=jnp.float32).astype(y_ref.dtype)


def place_kernel(index_ref, *refs):
    count = len(refs) // 2
    rows = refs[0].shape[0]
    target = pl.program_id(0) * BLK + lax.broadcasted_iota(jnp.int32, (BLK, rows), 0)
    chosen = jnp.where(target == index_ref[:1, :], 1.0, 0.0).astype(jnp.bfloat16)
    for x_ref, y_ref in zip(refs[:count], refs[count:]):
        y_ref[...] = jnp.dot(chosen, x_ref[...], preferred_element_type=jnp.float32).astype(y_ref.dtype)


def permuted(kernel, name, index_rows, *arrays):
    rows = arrays[0].shape[0]
    picks = kernel is pick_kernel
    index_spec = pl.BlockSpec((8, BLK), lambda i: (0, i)) if picks else pl.BlockSpec((8, rows), lambda i: (0, 0))
    return pl.pallas_call(
        kernel,
        out_shape=[jax.ShapeDtypeStruct(a.shape, a.dtype) for a in arrays],
        grid=(rows // BLK,),
        in_specs=[index_spec] + [pl.BlockSpec(a.shape, lambda i: (0, 0)) for a in arrays],
        out_specs=[pl.BlockSpec((BLK, a.shape[1]), lambda i: (i, 0)) for a in arrays],
        compiler_params=pltpu.CompilerParams(dimension_semantics=("arbitrary",), vmem_limit_bytes=24 << 20),
        cost_estimate=pl.CostEstimate(flops=2 * rows * rows * 256 * len(arrays), bytes_accessed=4 << 20, transcendentals=0),
        name=name,
    )(index_rows, *arrays)


def pick(index_rows, *arrays):
    return permuted(pick_kernel, "pick_rows", index_rows, *arrays)


def place(index_rows, *arrays):
    return permuted(place_kernel, "place_rows", index_rows, *arrays)


def route_tables(routing, rows):
    groups = routing.shape[0] // rows
    me = lax.axis_index("wide")
    ids = routing.reshape(groups, rows)
    positions = jnp.arange(rows, dtype=jnp.int32)
    beyond = jnp.int32(rows * rows)
    keys = jnp.where(ids // rows == me, positions[None, :] * rows + ids % rows, beyond)
    send = (jnp.sort(keys, axis=1)[:, : rows // groups] % rows).reshape(rows)
    own = lax.dynamic_index_in_dim(ids, me, 0, keepdims=False)
    arrive = jnp.sort(own // rows * rows + positions) % rows
    return jnp.broadcast_to(send[None], (8, rows)), jnp.broadcast_to(arrive[None], (8, rows))


def exchanged(rows_out):
    return lax.all_to_all(rows_out, "wide", split_axis=0, concat_axis=0, tiled=True)


def row_stats(rows_full):
    mean = jnp.mean(rows_full, axis=1, keepdims=True)
    scale = lax.rsqrt(jnp.mean(rows_full * rows_full, axis=1, keepdims=True) - mean * mean + NORM_EPS)
    return mean, scale


def local(
    inputs,
    cotangent,
    routing,
    lengths,
    ln1_gain,
    ln1_bias,
    qkv_weight,
    qv_bias,
    out_weight,
    out_bias,
    ln2_gain,
    ln2_bias,
    up_weight,
    up_bias,
    down_weight,
    down_bias,
):
    low, wide_type = jnp.bfloat16, jnp.float32
    row_count, quarter = inputs.shape
    parts = lax.axis_size("narrow")
    share = row_count // parts
    part = lax.axis_index("narrow")
    send_rows, arrive_rows = route_tables(routing, row_count)

    def mine(rows_full):
        return lax.dynamic_slice_in_dim(rows_full, part * share, share, 0)

    def my_features(rows_full):
        return lax.dynamic_slice_in_dim(rows_full, part * quarter, quarter, 1)

    (sent,) = pick(send_rows, inputs)
    (routed,) = place(arrive_rows, exchanged(sent))
    (sent_grad,) = pick(send_rows, cotangent)
    (routed_grad,) = place(arrive_rows, exchanged(sent_grad))
    vectors = jnp.stack([ln1_gain, ln1_bias, ln2_gain, ln2_bias, out_bias, down_bias])
    vectors = lax.all_gather(vectors, "narrow", axis=1, tiled=True)
    start, first = doc_tables(lengths[0], row_count)

    qkv_full = lax.all_gather(qkv_weight.astype(low).reshape(qkv_weight.shape[0], 3 * quarter), "wide", axis=0, tiled=True)
    out_full = lax.all_gather(out_weight.astype(low), "wide", axis=1, tiled=True)
    up_full = lax.all_gather(up_weight.astype(low), "wide", axis=0, tiled=True)
    down_full = lax.all_gather(down_weight.astype(low), "wide", axis=1, tiled=True)

    routed_low = lax.all_gather(routed, "narrow", axis=1, tiled=True)
    routed_full = routed_low.astype(wide_type)
    mean_one, scale_one = row_stats(routed_full)
    act_one = ((routed_full - mean_one) * scale_one * vectors[0] + vectors[1]).astype(low)
    shift = jnp.concatenate([qv_bias[0], jnp.zeros((quarter,), wide_type), qv_bias[1]])
    proj = (jnp.dot(act_one, qkv_full, preferred_element_type=wide_type) + shift).astype(low)
    mixed, log_sums = attention_forward(proj, first, jnp.broadcast_to(start[:, None], (row_count, 128)))
    norm_rows = jnp.concatenate([vectors[4:5], vectors[2:4], jnp.zeros((5, D), wide_type)])
    act_two, middle = project_and_norm(mixed, out_full, mine(routed_low), norm_rows)

    grad_full = lax.all_gather(routed_grad, "narrow", axis=1, tiled=True)
    hidden, grad_pre, branch_full, norm_sums = mlp_both_ways(
        act_two, grad_full, up_full, down_full, jnp.broadcast_to(up_bias[None], (8, up_bias.shape[0])), middle, norm_rows
    )

    held = jnp.arange(parts, dtype=jnp.int32)[:, None, None] == part
    kept = jnp.where(held, (middle + vectors[5])[None], 0.0).reshape(row_count, D)
    result = (jnp.dot(hidden, down_full, preferred_element_type=wide_type) + kept).astype(low)
    result = lax.psum_scatter(result, "narrow", scatter_dimension=1, tiled=True)
    down_grad = jnp.einsum("tf,td->fd", hidden, grad_full, preferred_element_type=wide_type).astype(low)
    up_grad = jnp.einsum("td,tf->df", act_two, grad_pre, preferred_element_type=wide_type).astype(low)
    down_grad = lax.psum_scatter(down_grad, "wide", scatter_dimension=1, tiled=True).astype(wide_type)
    up_grad = lax.psum_scatter(up_grad, "wide", scatter_dimension=0, tiled=True).astype(wide_type)

    out_grad = jnp.einsum("tf,td->fd", mixed, branch_full, preferred_element_type=wide_type).astype(low)
    out_grad = lax.psum_scatter(out_grad, "wide", scatter_dimension=1, tiled=True).astype(wide_type)
    grad_mixed = jnp.einsum("td,fd->tf", branch_full, out_full, preferred_element_type=wide_type).astype(low)
    grad_q, grad_k, grad_v = attention_backward(
        proj, mixed, grad_mixed, log_sums, first, jnp.broadcast_to(start[None], (8, row_count))
    )
    grad_proj = jnp.concatenate([grad_q, grad_k, grad_v], axis=1)
    grad_act_one = jnp.einsum("tc,dc->td", grad_proj, qkv_full, preferred_element_type=wide_type).astype(low)
    grad_act_one = lax.psum_scatter(grad_act_one, "narrow", scatter_dimension=1, tiled=True).astype(wide_type)
    qkv_grad = jnp.einsum("td,tc->dc", act_one, grad_proj, preferred_element_type=wide_type).astype(low)
    qkv_grad = lax.psum_scatter(qkv_grad, "wide", scatter_dimension=0, tiled=True).astype(wide_type)

    normed_one = (routed.astype(wide_type) - mean_one) * scale_one
    scaled = grad_act_one * ln1_gain
    totals = lax.psum(jnp.stack([jnp.sum(scaled, axis=1), jnp.sum(scaled * normed_one, axis=1)]), "narrow") / D
    back_one = scale_one * (scaled - totals[0][:, None] - normed_one * totals[1][:, None])
    grad_input = (my_features(branch_full).astype(wide_type) + back_one).astype(low)

    (result_sent,) = pick(arrive_rows, result)
    (outputs,) = place(send_rows, exchanged(result_sent))
    (input_sent,) = pick(arrive_rows, grad_input)
    (input_grad,) = place(send_rows, exchanged(input_sent))

    norm_two = lax.psum(norm_sums[:2], ("wide", "narrow"))
    norm_two = lax.dynamic_slice_in_dim(norm_two, part * quarter, quarter, 1)
    middle_sums = lax.psum(
        (
            jnp.sum(my_features(branch_full), axis=0, dtype=wide_type),
            jnp.sum(grad_pre, axis=0, dtype=wide_type),
            jnp.sum(routed_grad, axis=0, dtype=wide_type),
        ),
        "wide",
    )
    last_sums = lax.psum(
        (
            jnp.sum(grad_act_one * normed_one, axis=0),
            jnp.sum(grad_act_one, axis=0),
            jnp.stack([jnp.sum(grad_q, axis=0, dtype=wide_type), jnp.sum(grad_v, axis=0, dtype=wide_type)]),
        ),
        "wide",
    )
    return (
        outputs,
        input_grad,
        last_sums[0],
        last_sums[1],
        qkv_grad.reshape(qkv_weight.shape),
        last_sums[2],
        out_grad,
        middle_sums[0],
        norm_two[0],
        norm_two[1],
        up_grad,
        middle_sums[1],
        down_grad,
        middle_sums[2],
    )


def solution(mesh):
    row_mat, col_mat, vector = P("wide", "narrow"), P("narrow", "wide"), P("narrow")
    projections, pair = P("wide", None, "narrow"), P(None, "narrow")
    return jax.shard_map(
        local,
        mesh=mesh,
        in_specs=(
            row_mat,
            row_mat,
            P(),
            P("wide", None),
            vector,
            vector,
            projections,
            pair,
            col_mat,
            vector,
            vector,
            vector,
            row_mat,
            vector,
            col_mat,
            vector,
        ),
        out_specs=(
            row_mat,
            row_mat,
            vector,
            vector,
            projections,
            pair,
            col_mat,
            vector,
            vector,
            vector,
            row_mat,
            vector,
            col_mat,
            vector,
        ),
        check_vma=False,
    )
```
